32 devices in a mesh: outer: 4 (over y, x), rep: 4 (over z), shard: 2 (over core).
Axes of the slice: x: 2, y: 2, z: 4, core: 2. Of those that a mesh axis runs over, the one named last changes fastest.
Arguments:
- deltas: bfloat16 [4, 4, 1024, 5120], P('outer', 'rep', 'shard'), may hold values from -1400 to 1400, as said below
- owners: int32 [2, 4, 1], P('shard'), may hold values from 0 to 3; in each aligned block of 4 rows (0 to 3, 4 to 7, ..., all dimensions but the last counted through in order) at most 2 rows name the same one
- master: float32 [4, 2, 2, 128, 5120], P('outer', 'shard', None, 'rep'), may hold values from -6 to 6
- momentum: float32 [4, 2, 2, 128, 5120], P('outer', 'shard', None, 'rep'), may hold values from -3 to 3
Outputs:
- new_params: bfloat16 [1024, 5120], P('shard')
- new_momentum: float32 [4, 2, 2, 128, 5120], P('outer', 'shard', None, 'rep')
- new_master: float32 [4, 2, 2, 128, 5120], P('outer', 'shard', None, 'rep')
The draws below stay inside these ranges and needn't reach their ends.
Inputs may be any that keep to these rules, and one draw needn't show every extreme that they name: `owners`: within each shard, no pod owns more than 2 blocks, and in some shards one pod owns exactly 2. `deltas`: finite values.
All inputs are finite; a program needn't handle non-finite values.
Results may differ from the reference program's by a relative error of at most 0.0075.
Values may be sent and summed in bfloat16 or wider, within the bound.
A program may use at most 128 MiB of HBM per device.

```python
import math
import jax
import jax.numpy as jnp
import numpy as np
from jax import lax

D = 5120
BLOCK_ROWS = 128
BLOCKS = 4
MOST = 2
N_OUTER = 4
N_REP = 4
N_SHARD = 2


def draw_deltas(key, part):
    total_rows = N_SHARD * BLOCKS * BLOCK_ROWS
    noise_key, row_key, col_key = jax.random.split(key, 3)
    position = jnp.arange(total_rows, dtype=jnp.float32) / (total_rows - 1.0)
    noise = jnp.clip(jax.random.normal(noise_key, (N_OUTER, N_REP, total_rows, D), jnp.float32), -5.0, 5.0)
    ramp = 1.0 + 2.0 * position
    row_scale = jnp.exp(jax.random.uniform(row_key, (N_OUTER, N_REP, total_rows, 1), jnp.float32, 0.0, 2.302585))
    col_scale = jnp.exp(jax.random.uniform(col_key, (1, 1, 1, D), jnp.float32, 0.0, 1.098612))
    values = noise * row_scale * col_scale * ramp[None, None, :, None]
    return values.astype(jnp.bfloat16)


def shard_levels(key, extent, cuts, least, high):
    def one(dim, shards_of):
        draws = jax.random.uniform(jax.random.fold_in(jax.random.fold_in(key, 6), dim), (shards_of,), jnp.float32, least / len(cuts), high / len(cuts))
        return jnp.repeat(jnp.exp(draws), extent[dim] // shards_of).reshape((-1,) + (1,) * (len(extent) - dim - 1))

    factor_of = one(*cuts[0])
    for cut in cuts[1:]:
        factor_of = factor_of * one(*cut)
    return factor_of


def routed_block(stream_key, own, number, rows, count, top, bound, lean):
    ranking = jax.random.permutation(stream_key, count)
    crowded, usual = shares(count, rows * top, bound, lean, True), shares(count, rows * top, bound, lean, False)
    places = jnp.arange(count)

    def named(tallies, offset_by):
        used = int((tallies > 0).sum())
        fixed = max(1, used // 4)
        moved = fixed + (places - fixed + offset_by * (used - fixed)) % max(1, count - fixed)
        return jnp.zeros((count,), jnp.int32).at[ranking[jnp.where(places < fixed, places, moved)]].set(jnp.asarray(tallies, jnp.int32))

    tallies = jnp.where(number % 4 == 0, named(crowded, number // 4), named(usual, number - number // 4 - 1))
    mixed = jax.random.permutation(jax.random.fold_in(own, 3), count)
    giver, taker = mixed[0:count // 2 * 2:2], mixed[1:count // 2 * 2:2]
    room = jnp.minimum(tallies[giver] - 1, bound - tallies[taker]) // 2
    room = jnp.where((giver == ranking[0]) | (taker == ranking[0]) | (tallies[taker] == 0), 0, jnp.maximum(room, 0))
    moved = jax.random.randint(jax.random.fold_in(own, 4), (count // 2,), 0, 1 << 20) % (room + 1)
    tallies = tallies.at[giver].add(-moved).at[taker].add(moved)
    labels = jnp.searchsorted(jnp.cumsum(tallies), jnp.arange(rows * top), side="right").astype(jnp.int32)
    grid = labels.reshape(top, rows).T
    grid = grid[jax.random.permutation(jax.random.fold_in(own, 1), rows)]
    offset_by = jax.random.randint(jax.random.fold_in(own, 2), (rows, 1), 0, top)
    return jnp.take_along_axis(grid, (jnp.arange(top)[None, :] + offset_by) % top, axis=1)


def shares(amount, total, limit, lean, full):
    weights = [(1 << 20) // math.isqrt(grade ** lean) + 1 for grade in range(1, amount + 1)]
    largest = limit if full else min(limit, max(-(-total // amount), total * weights[0] // sum(weights)))
    least = 1 if total - largest >= amount - 1 else 0
    holding, rest = [largest] + [least] * (amount - 1), total - largest - least * (amount - 1)
    while rest > 0:
        candidates = [i for i in range(1, amount) if holding[i] < largest] or [i for i in range(1, amount) if holding[i] < limit]
        pool, budget = sum([weights[i] for i in candidates]), rest
        for i in candidates:
            extra = min(limit - holding[i], max(1, budget * weights[i] // pool), rest)
            holding[i] = holding[i] + extra
            rest = rest - extra
    return np.array(holding)


def bell_draw(key, extent, spread, bound, shards=(), held_as=jnp.bfloat16):
    values = jax.random.normal(key, extent, jnp.float32) * spread
    if len(shards) > 0:
        values = shard_levels(key, extent, shards, -0.22, 0.18) * values
    return jnp.clip(values, min=-bound, max=bound).astype(held_as)


def setup_inputs(seed: int = 0) -> dict:
    arg_keys = jax.random.split(jax.random.key(seed), 5)
    deltas = draw_deltas(jax.random.fold_in(arg_keys[4], 71), 0)
    owners_keys = jax.random.split(jax.random.fold_in(arg_keys[1], 1), N_SHARD * BLOCKS // BLOCKS)
    owners_turns = jax.random.permutation(jax.random.fold_in(arg_keys[1], 3), N_SHARD * BLOCKS // BLOCKS)
    owners = jax.vmap(lambda own, number: routed_block(jax.random.fold_in(arg_keys[1], 2), own, number, BLOCKS, N_OUTER, 1, MOST, 2))(owners_keys, owners_turns).reshape((N_SHARD, BLOCKS, 1))
    master = bell_draw(arg_keys[2], (N_OUTER, N_SHARD, MOST, BLOCK_ROWS, D), 1.0, 6.0, ((0, 4), (1, 2), (3, 4)), jnp.float32)
    momentum = bell_draw(arg_keys[3], (N_OUTER, N_SHARD, MOST, BLOCK_ROWS, D), 0.5, 3.0, ((0, 4), (1, 2), (3, 4)), jnp.float32)
    return dict(deltas=deltas, owners=owners, master=master, momentum=momentum)


def reference(deltas, owners, master, momentum):
    total_reps = N_OUTER * N_REP
    pod_sums = lax.optimization_barrier(jnp.sum(deltas.astype(jnp.float32), axis=1)).astype(jnp.bfloat16)
    mean_delta = lax.optimization_barrier(jnp.sum(pod_sums.astype(jnp.float32), axis=0)) / total_reps
    owned_blocks = owners[:, :, 0].astype(jnp.int32)
    pod_ids = jnp.arange(N_OUTER, dtype=jnp.int32)
    onehot = (owned_blocks[:, :, None] == pod_ids[None, None, :]).astype(jnp.int32)
    rank_all = jnp.cumsum(onehot, axis=1) - onehot
    rank_own = lax.optimization_barrier(jnp.sum(rank_all * onehot, axis=2))
    slot_ids = jnp.arange(MOST, dtype=jnp.int32)
    selector = ((owned_blocks[None, :, None, :] == pod_ids[:, None, None, None]) & (rank_own[None, :, None, :] == slot_ids[None, None, :, None])).astype(jnp.float32)
    blocks = mean_delta.reshape(N_SHARD, BLOCKS, BLOCK_ROWS, D)
    slotted = jnp.einsum('osjb,sbrw->osjrw', selector, blocks, precision=lax.Precision.HIGHEST)
    sum_squares = jnp.sum(mean_delta * mean_delta)
    clip_limit = 0.5 * math.sqrt(N_SHARD * BLOCKS * BLOCK_ROWS * D)
    factor = jnp.minimum(1.0, clip_limit / jnp.sqrt(sum_squares + 1e-06))
    new_momentum = 0.9 * momentum + factor * slotted
    new_master = master - 0.7 * (factor * slotted + 0.9 * new_momentum)
    restored = jnp.einsum('osjb,osjrw->sbrw', selector, new_master, precision=lax.Precision.HIGHEST)
    new_params = restored.reshape(N_SHARD * BLOCKS * BLOCK_ROWS, D).astype(jnp.bfloat16)
    return (new_params, new_momentum, new_master)
```

```python
import functools
import math

import jax
import jax.numpy as jnp
from jax import lax
from jax.experimental import pallas as pl
from jax.experimental.pallas import tpu as pltpu
from jax.sharding import PartitionSpec as P

CHUNKS = 4
TILE = 16
SIDE = 2


def ranks(owners, pod_count):
    owned_blocks = owners[0, :, 0]
    pod_ids = jnp.arange(pod_count, dtype=jnp.int32)
    onehot = (owned_blocks[:, None] == pod_ids[None, :]).astype(jnp.int32)
    rank_all = jnp.cumsum(onehot, axis=0) - onehot
    return owned_blocks, jnp.sum(rank_all * onehot, axis=1)


def kernel(
    chunks, rep_count, shard_count, clip_limit,
    sel, deltas, master, momentum,
    out, new_momentum, new_master,
    first, kept, passed, second, summed, third, mean, contrib, fourth, squares, others,
    send_sem, recv_sem,
):
    blocks, slots, sub_rows, width = contrib.shape[0], master.shape[0], master.shape[1], master.shape[2]
    block_rows = deltas.shape[2]
    pod_count = SIDE * SIDE
    half = width // 2
    cols = half // chunks
    o, q, s = lax.axis_index("outer"), lax.axis_index("rep"), lax.axis_index("shard")
    y, x = o // SIDE, o % SIDE
    x_pod, y_pod = y * SIDE + 1 - x, (1 - y) * SIDE + x

    def pod(d):
        return ((y + d // SIDE) % SIDE) * SIDE + (x + d % SIDE) % SIDE

    barrier = pltpu.get_barrier_semaphore()
    peers = [{"outer": pod(d)} for d in range(1, pod_count)]
    peers += [{"rep": (q + d) % rep_count} for d in range(1, rep_count)]
    peers += [{"shard": (s + d) % shard_count} for d in range(1, shard_count)]
    for peer in peers:
        pl.semaphore_signal(barrier, inc=1, device_id=peer, device_id_type=pl.DeviceIdType.MESH)
    pl.semaphore_wait(barrier, len(peers))

    started = []

    def send(src, dst, **to):
        number = len(started)
        copy = pltpu.make_async_remote_copy(
            src_ref=src, dst_ref=dst, send_sem=send_sem.at[number], recv_sem=recv_sem.at[number],
            device_id=to, device_id_type=pl.DeviceIdType.MESH,
        )
        copy.start()
        started.append(copy)
        return copy

    def tiles(rows, body):
        def step(i, carry):
            body(pl.ds(pl.multiple_of(i * TILE, TILE), TILE))
            return carry

        lax.fori_loop(0, rows // TILE, step, 0)

    def left(c):
        return pl.ds(c * cols, cols)

    def right(c):
        return pl.ds(half + c * cols, cols)

    def pair(c):
        return (left(c), right(c))

    flight = {}

    def send_first(c):
        l, r = pair(c)
        flight["first", c] = [
            send(deltas.at[:, 1 - x, :, l], first.at[:, :, l], outer=x_pod),
            send(deltas.at[1 - y, :, :, r], first.at[:, :, r], outer=y_pod),
        ]

    def send_second(c):
        for copy in flight["first", c]:
            copy.wait_recv()
        l, r = pair(c)

        def body(rows):
            for at, go, stay in ((l, 1 - y, y), (r, 1 - x, x)):
                own = (lambda k: deltas[k, x, rows, at]) if at is l else (lambda k: deltas[y, k, rows, at])
                passed[rows, at] = (
                    own(go).astype(jnp.float32) + first[go, rows, at].astype(jnp.float32)
                ).astype(jnp.bfloat16)
                kept[rows, at] = own(stay).astype(jnp.float32) + first[stay, rows, at].astype(jnp.float32)

        tiles(block_rows, body)
        flight["second", c] = [
            send(passed.at[:, l], second.at[:, l], outer=y_pod),
            send(passed.at[:, r], second.at[:, r], outer=x_pod),
        ]

    def send_third(c):
        for copy in flight["second", c]:
            copy.wait_recv()

        def body(rows):
            for at in pair(c):
                total = kept[rows, at] + second[rows, at].astype(jnp.float32)
                kept[rows, at] = total
                summed[rows, at] = total.astype(jnp.bfloat16)

        tiles(block_rows, body)
        flight["third", c] = []
        for at in pair(c):
            for d in range(1, rep_count):
                there = (q + d) % rep_count
                rows = pl.ds(pl.multiple_of(there * sub_rows, sub_rows), sub_rows)
                flight["third", c].append(send(summed.at[rows, at], third.at[d - 1, :, at], rep=there))

    def take_mean(c):
        for copy in flight["third", c]:
            copy.wait_recv()

        def body(rows):
            mine = pl.ds(pl.multiple_of(q * sub_rows + rows.start, TILE), TILE)
            for at in pair(c):
                total = kept[mine, at]
                for d in range(rep_count - 1):
                    total = total + third[d, rows, at].astype(jnp.float32)
                value = total * (1.0 / (pod_count * rep_count))
                mean[o, rows, at] = value.astype(jnp.bfloat16)
                square = value * value
                part = squares[0]
                for i in range(cols // 128):
                    for k in range(TILE // 8):
                        part = part + square[k * 8:(k + 1) * 8, i * 128:(i + 1) * 128]
                squares[0] = part

        tiles(sub_rows, body)

    def send_mean(c):
        flight["mean", c] = [
            send(mean.at[o, :, at], mean.at[o, :, at], outer=pod(d))
            for at in pair(c) for d in range(1, pod_count)
        ]

    squares[0] = jnp.zeros(squares.shape[1:], jnp.float32)
    send_first(0)
    send_first(1)
    for t in range(chunks + 2):
        if t < chunks:
            send_second(t)
        if t + 2 < chunks:
            send_first(t + 2)
        if 0 <= t - 1 < chunks:
            send_third(t - 1)
        if 0 <= t - 2 < chunks:
            take_mean(t - 2)
            if t - 2 < chunks - 1:
                send_mean(t - 2)

    number = 0
    for level, (axis, count) in enumerate((("shard", shard_count), ("rep", rep_count), ("outer", pod_count))):
        copies = []
        for d in range(1, count):
            there = {"shard": (s + d) % shard_count, "rep": (q + d) % rep_count, "outer": pod(d)}[axis]
            copies.append(send(squares.at[level], others.at[number + d - 1], **{axis: there}))
        if level == 0:
            send_mean(chunks - 1)
        total = squares[level]
        for d, copy in enumerate(copies):
            copy.wait_recv()
            total = total + others[number + d]
        number += count - 1
        squares[level + 1] = total
    total = jnp.sum(squares[3], keepdims=True)
    factor = jnp.minimum(1.0, clip_limit / jnp.sqrt(total + 1e-06))

    def update(c):
        for copy in flight["mean", c]:
            copy.wait_recv()

        def body(rows):
            for at in pair(c):
                steps = [factor * mean[b, rows, at].astype(jnp.float32) for b in range(blocks)]
                masters = []
                for j in range(slots):
                    step = sum(sel[b, j] * steps[b] for b in range(blocks))
                    moved = 0.9 * momentum[j, rows, at] + step
                    new_momentum[j, rows, at] = moved
                    value = master[j, rows, at] - 0.7 * (step + 0.9 * moved)
                    new_master[j, rows, at] = value
                    masters.append(value)
                for b in range(blocks):
                    value = sum(sel[b, j] * masters[j] for j in range(slots))
                    contrib[b, rows, at] = value.astype(jnp.bfloat16)

        tiles(sub_rows, body)
        flight["fourth", c] = []
        for at in pair(c):
            for d in range(1, pod_count):
                flight["fourth", c].append(
                    send(contrib.at[pod(d), :, at], fourth.at[d - 1, :, at], outer=pod(d))
                )

    def send_rows(c):
        for copy in flight["fourth", c]:
            copy.wait_recv()

        def body(rows):
            mine = pl.ds(pl.multiple_of(q * sub_rows + rows.start, TILE), TILE)
            for at in pair(c):
                value = contrib[o, rows, at].astype(jnp.float32)
                for d in range(pod_count - 1):
                    value = value + fourth[d, rows, at].astype(jnp.float32)
                out[y, x, mine, at] = value.astype(jnp.bfloat16)

        tiles(sub_rows, body)
        rows = pl.ds(pl.multiple_of(q * sub_rows, sub_rows), sub_rows)
        flight["rows", c] = [
            send(out.at[y, x, rows, at], out.at[y, x, rows, at], rep=(q + d) % rep_count)
            for at in pair(c) for d in range(1, rep_count)
        ]

    def send_block(c):
        for copy in flight["rows", c]:
            copy.wait_recv()
        l, r = pair(c)
        flight["block", c] = [
            send(out.at[y, x, :, l], out.at[y, x, :, l], outer=x_pod),
            send(out.at[y, x, :, r], out.at[y, x, :, r], outer=y_pod),
        ]

    def send_blocks(c):
        for copy in flight["block", c]:
            copy.wait_recv()
        l, r = pair(c)
        flight["blocks", c] = [
            send(out.at[y, :, :, l], out.at[y, :, :, l], outer=y_pod),
            send(out.at[:, x, :, r], out.at[:, x, :, r], outer=x_pod),
        ]

    for t in range(chunks + 3):
        for lag, stage in enumerate((update, send_rows, send_block, send_blocks)):
            if 0 <= t - lag < chunks:
                stage(t - lag)
    for c in range(chunks):
        for copy in flight["blocks", c]:
            copy.wait_recv()
    for copy in started:
        copy.wait_send()


def fused(deltas, owners, master, momentum):
    blocks = owners.shape[1]
    slots, sub_rows, width = master.shape[2:]
    block_rows = deltas.shape[2] // blocks
    pod_count, rep_count = lax.axis_size("outer"), lax.axis_size("rep")
    owned_blocks, rank_own = ranks(owners, pod_count)
    mine = owned_blocks == lax.axis_index("outer")
    sel = (mine[:, None] & (rank_own[:, None] == jnp.arange(slots)[None, :])).astype(jnp.float32)
    clip_limit = 0.5 * math.sqrt(lax.axis_size("shard") * blocks * block_rows * width)
    copies = CHUNKS * (4 + 2 * (rep_count - 1) + 4 * (pod_count - 1) + 2 * (rep_count - 1) + 4)
    exchanged = lax.axis_size("shard") + rep_count + pod_count - 3
    copies += exchanged
    vmem = pl.BlockSpec(memory_space=pltpu.VMEM)
    bf16, f32 = jnp.bfloat16, jnp.float32
    out, new_momentum, new_master = pl.pallas_call(
        functools.partial(kernel, CHUNKS, rep_count, lax.axis_size("shard"), clip_limit),
        out_shape=(
            jax.ShapeDtypeStruct((SIDE, SIDE, block_rows, width), bf16),
            jax.ShapeDtypeStruct(master.shape[2:], f32),
            jax.ShapeDtypeStruct(master.shape[2:], f32),
        ),
        in_specs=[pl.BlockSpec(memory_space=pltpu.SMEM), vmem, vmem, vmem],
        out_specs=(vmem, vmem, vmem),
        scratch_shapes=[
            pltpu.VMEM((SIDE, block_rows, width), bf16),
            pltpu.VMEM((block_rows, width), f32),
            pltpu.VMEM((block_rows, width), bf16),
            pltpu.VMEM((block_rows, width), bf16),
            pltpu.VMEM((block_rows, width), bf16),
            pltpu.VMEM((rep_count - 1, sub_rows, width), bf16),
            pltpu.VMEM((blocks, sub_rows, width), bf16),
            pltpu.VMEM((blocks, sub_rows, width), bf16),
            pltpu.VMEM((pod_count - 1, sub_rows, width), bf16),
            pltpu.VMEM((4, 8, 128), f32),
            pltpu.VMEM((exchanged, 8, 128), f32),
            pltpu.SemaphoreType.DMA((copies,)),
            pltpu.SemaphoreType.DMA((copies,)),
        ],
        compiler_params=pltpu.CompilerParams(
            collective_id=0, has_side_effects=True, vmem_limit_bytes=60 * 1024 * 1024
        ),
    )(
        sel,
        deltas.reshape(SIDE, SIDE, block_rows, width),
        master.reshape(master.shape[2:]),
        momentum.reshape(momentum.shape[2:]),
    )
    return (
        out.reshape(blocks * block_rows, width),
        new_momentum.reshape(momentum.shape),
        new_master.reshape(master.shape),
    )


def local(deltas, owners, master, momentum):
    blocks_here = owners.shape[1]
    slot_count = master.shape[2]
    sub_rows = master.shape[3]
    row_width = deltas.shape[3]
    block_rows = deltas.shape[2] // blocks_here
    pod_count = lax.axis_size("outer")
    rep_count = lax.axis_size("rep")
    owned_blocks = owners[0, :, 0]
    pod_ids = jnp.arange(pod_count, dtype=jnp.int32)
    onehot = (owned_blocks[:, None] == pod_ids[None, :]).astype(jnp.int32)
    rank_all = jnp.cumsum(onehot, axis=0) - onehot
    rank_own = jnp.sum(rank_all * onehot, axis=1)
    slot_ids = jnp.arange(slot_count, dtype=jnp.int32)
    selector = (
        (owned_blocks[None, None, :] == pod_ids[:, None, None])
        & (rank_own[None, None, :] == slot_ids[None, :, None])
    ).astype(jnp.bfloat16)
    local_rows = deltas[0, 0].reshape(blocks_here, block_rows, row_width)
    block_sums = lax.psum_scatter(
        local_rows.astype(jnp.float32).astype(jnp.bfloat16), "rep", scatter_dimension=1, tiled=True
    ).astype(jnp.float32)
    block_sums = block_sums.astype(jnp.bfloat16)
    pod_part = jnp.einsum(
        "ojb,brw->ojrw", selector, block_sums, preferred_element_type=jnp.float32
    ).astype(jnp.bfloat16)
    arrived = lax.all_to_all(pod_part, "outer", split_axis=0, concat_axis=0, tiled=True)
    mean_share = jnp.sum(arrived.astype(jnp.float32), axis=0) / (pod_count * rep_count)
    local_sq = jnp.sum(mean_share * mean_share)
    total_sq = lax.psum(local_sq, ("outer", "rep", "shard"))
    total_entries = lax.axis_size("shard") * blocks_here * block_rows * row_width
    clip_limit = 0.5 * math.sqrt(total_entries)
    factor = jnp.minimum(1.0, clip_limit / jnp.sqrt(total_sq + 1e-06))
    step_part = factor * mean_share[None, None]
    new_momentum = 0.9 * momentum + step_part
    new_master = master - 0.7 * (step_part + 0.9 * new_momentum)
    params_here = new_master.astype(jnp.bfloat16)
    gathered = lax.all_gather(params_here, ("outer", "rep"), axis=0, tiled=True).reshape(
        pod_count, rep_count, slot_count, sub_rows, row_width
    )
    unpacked = jnp.einsum("ojb,oqjrw->bqrw", selector, gathered, preferred_element_type=jnp.float32)
    new_params = unpacked.astype(jnp.bfloat16).reshape(blocks_here * block_rows, row_width)
    return (new_params, new_momentum, new_master)


def solution(mesh):
    fits = mesh.shape["outer"] == SIDE * SIDE

    def body(deltas, owners, master, momentum):
        blocks = owners.shape[1]
        width, sub_rows = master.shape[4], master.shape[3]
        whole = width % (2 * CHUNKS * 128) == 0 and sub_rows % TILE == 0
        plan = fused if fits and whole and blocks == SIDE * SIDE else local
        return plan(deltas, owners, master, momentum)

    return jax.shard_map(
        body,
        mesh=mesh,
        in_specs=(
            P("outer", "rep", "shard", None),
            P("shard", None, None),
            P("outer", "shard", None, "rep", None),
            P("outer", "shard", None, "rep", None),
        ),
        out_specs=(
            P("shard", None),
            P("outer", "shard", None, "rep", None),
            P("outer", "shard", None, "rep", None),
        ),
        check_vma=False,
    )
```

```python
import functools
import math

import jax
import jax.numpy as jnp
from jax import lax
from jax.experimental import pallas as pl
from jax.experimental.pallas import tpu as pltpu
from jax.sharding import PartitionSpec as P

CHUNKS = 5
TILE = 16
SIDE = 2


def ranks(owners, pod_count):
    owned_blocks = owners[0, :, 0]
    pod_ids = jnp.arange(pod_count, dtype=jnp.int32)
    onehot = (owned_blocks[:, None] == pod_ids[None, :]).astype(jnp.int32)
    rank_all = jnp.cumsum(onehot, axis=0) - onehot
    return owned_blocks, jnp.sum(rank_all * onehot, axis=1)


def kernel(
    chunks, rep_count, shard_count, clip_limit,
    sel, deltas, master, momentum,
    out, new_momentum, new_master,
    first, kept, passed, second, summed, third, mean, contrib, fourth, squares, others,
    send_sem, recv_sem,
):
    blocks, slots, sub_rows, width = contrib.shape[0], master.shape[0], master.shape[1], master.shape[2]
    block_rows = deltas.shape[2]
    pod_count = SIDE * SIDE
    half = width // 2
    cols = half // chunks
    o, q, s = lax.axis_index("outer"), lax.axis_index("rep"), lax.axis_index("shard")
    y, x = o // SIDE, o % SIDE
    x_pod, y_pod = y * SIDE + 1 - x, (1 - y) * SIDE + x

    def pod(d):
        return ((y + d // SIDE) % SIDE) * SIDE + (x + d % SIDE) % SIDE

    barrier = pltpu.get_barrier_semaphore()
    peers = [{"outer": pod(d)} for d in range(1, pod_count)]
    peers += [{"rep": (q + d) % rep_count} for d in range(1, rep_count)]
    peers += [{"shard": (s + d) % shard_count} for d in range(1, shard_count)]
    for peer in peers:
        pl.semaphore_signal(barrier, inc=1, device_id=peer, device_id_type=pl.DeviceIdType.MESH)
    pl.semaphore_wait(barrier, len(peers))

    started = []

    def send(src, dst, **to):
        number = len(started)
        copy = pltpu.make_async_remote_copy(
            src_ref=src, dst_ref=dst, send_sem=send_sem.at[number], recv_sem=recv_sem.at[number],
            device_id=to, device_id_type=pl.DeviceIdType.MESH,
        )
        copy.start()
        started.append(copy)
        return copy

    def tiles(rows, body):
        def step(i, carry):
            body(pl.ds(pl.multiple_of(i * TILE, TILE), TILE))
            return carry

        lax.fori_loop(0, rows // TILE, step, 0)

    def left(c):
        return pl.ds(c * cols, cols)

    def right(c):
        return pl.ds(half + c * cols, cols)

    def pair(c):
        return (left(c), right(c))

    flight = {}

    def send_first(c):
        l, r = pair(c)
        flight["first", c] = [
            send(deltas.at[:, 1 - x, :, l], first.at[:, :, l], outer=x_pod),
            send(deltas.at[1 - y, :, :, r], first.at[:, :, r], outer=y_pod),
        ]

    def send_second(c):
        for copy in flight["first", c]:
            copy.wait_recv()
        l, r = pair(c)

        def body(rows):
            for at, go, stay in ((l, 1 - y, y), (r, 1 - x, x)):
                own = (lambda k: deltas[k, x, rows, at]) if at is l else (lambda k: deltas[y, k, rows, at])
                passed[rows, at] = (
                    own(go).astype(jnp.float32) + first[go, rows, at].astype(jnp.float32)
                ).astype(jnp.bfloat16)
                kept[rows, at] = own(stay).astype(jnp.float32) + first[stay, rows, at].astype(jnp.float32)

        tiles(block_rows, body)
        flight["second", c] = [
            send(passed.at[:, l], second.at[:, l], outer=y_pod),
            send(passed.at[:, r], second.at[:, r], outer=x_pod),
        ]

    def send_third(c):
        for copy in flight["second", c]:
            copy.wait_recv()

        def body(rows):
            for at in pair(c):
                total = kept[rows, at] + second[rows, at].astype(jnp.float32)
                kept[rows, at] = total
                summed[rows, at] = total.astype(jnp.bfloat16)

        tiles(block_rows, body)
        flight["third", c] = []
        for at in pair(c):
            for d in range(1, rep_count):
                there = (q + d) % rep_count
                rows = pl.ds(pl.multiple_of(there * sub_rows, sub_rows), sub_rows)
                flight["third", c].append(send(summed.at[rows, at], third.at[d - 1, :, at], rep=there))

    def take_mean(c):
        for copy in flight["third", c]:
            copy.wait_recv()

        def body(rows):
            mine = pl.ds(pl.multiple_of(q * sub_rows + rows.start, TILE), TILE)
            for at in pair(c):
                total = kept[mine, at]
                for d in range(rep_count - 1):
                    total = total + third[d, rows, at].astype(jnp.float32)
                value = total * (1.0 / (pod_count * rep_count))
                mean[o, rows, at] = value.astype(jnp.bfloat16)
                square = value * value
                part = squares[0]
                for i in range(cols // 128):
                    for k in range(TILE // 8):
                        part = part + square[k * 8:(k + 1) * 8, i * 128:(i + 1) * 128]
                squares[0] = part

        tiles(sub_rows, body)

    def send_mean(c):
        flight["mean", c] = [
            send(mean.at[o, :, at], mean.at[o, :, at], outer=pod(d))
            for at in pair(c) for d in range(1, pod_count)
        ]

    squares[0] = jnp.zeros(squares.shape[1:], jnp.float32)
    send_first(0)
    send_first(1)
    for t in range(chunks + 2):
        if t < chunks:
            send_second(t)
        if t + 2 < chunks:
            send_first(t + 2)
        if 0 <= t - 1 < chunks:
            send_third(t - 1)
        if 0 <= t - 2 < chunks:
            take_mean(t - 2)
            if t - 2 < chunks - 1:
                send_mean(t - 2)

    number = 0
    for level, (axis, count) in enumerate((("shard", shard_count), ("rep", rep_count), ("outer", pod_count))):
        copies = []
        for d in range(1, count):
            there = {"shard": (s + d) % shard_count, "rep": (q + d) % rep_count, "outer": pod(d)}[axis]
            copies.append(send(squares.at[level], others.at[number + d - 1], **{axis: there}))
        if level == 0:
            send_mean(chunks - 1)
        total = squares[level]
        for d, copy in enumerate(copies):
            copy.wait_recv()
            total = total + others[number + d]
        number += count - 1
        squares[level + 1] = total
    total = jnp.sum(squares[3], keepdims=True)
    factor = jnp.minimum(1.0, clip_limit / jnp.sqrt(total + 1e-06))

    def update(c):
        for copy in flight["mean", c]:
            copy.wait_recv()

        def body(rows):
            for at in pair(c):
                steps = [factor * mean[b, rows, at].astype(jnp.float32) for b in range(blocks)]
                masters = []
                for j in range(slots):
                    step = sum(sel[b, j] * steps[b] for b in range(blocks))
                    moved = 0.9 * momentum[j, rows, at] + step
                    new_momentum[j, rows, at] = moved
                    value = master[j, rows, at] - 0.7 * (step + 0.9 * moved)
                    new_master[j, rows, at] = value
                    masters.append(value)
                for b in range(blocks):
                    value = sum(sel[b, j] * masters[j] for j in range(slots))
                    contrib[b, rows, at] = value.astype(jnp.bfloat16)

        tiles(sub_rows, body)
        flight["fourth", c] = []
        for at in pair(c):
            for d in range(1, pod_count):
                flight["fourth", c].append(
                    send(contrib.at[pod(d), :, at], fourth.at[d - 1, :, at], outer=pod(d))
                )

    def send_rows(c):
        for copy in flight["fourth", c]:
            copy.wait_recv()

        def body(rows):
            mine = pl.ds(pl.multiple_of(q * sub_rows + rows.start, TILE), TILE)
            for at in pair(c):
                value = contrib[o, rows, at].astype(jnp.float32)
                for d in range(pod_count - 1):
                    value = value + fourth[d, rows, at].astype(jnp.float32)
                out[y, x, mine, at] = value.astype(jnp.bfloat16)

        tiles(sub_rows, body)
        rows = pl.ds(pl.multiple_of(q * sub_rows, sub_rows), sub_rows)
        flight["rows", c] = [
            send(out.at[y, x, rows, at], out.at[y, x, rows, at], rep=(q + d) % rep_count)
            for at in pair(c) for d in range(1, rep_count)
        ]

    def send_block(c):
        for copy in flight["rows", c]:
            copy.wait_recv()
        l, r = pair(c)
        flight["block", c] = [
            send(out.at[y, x, :, l], out.at[y, x, :, l], outer=x_pod),
            send(out.at[y, x, :, r], out.at[y, x, :, r], outer=y_pod),
        ]

    def send_blocks(c):
        for copy in flight["block", c]:
            copy.wait_recv()
        l, r = pair(c)
        flight["blocks", c] = [
            send(out.at[y, :, :, l], out.at[y, :, :, l], outer=y_pod),
            send(out.at[:, x, :, r], out.at[:, x, :, r], outer=x_pod),
        ]

    for t in range(chunks + 3):
        for lag, stage in enumerate((update, send_rows, send_block, send_blocks)):
            if 0 <= t - lag < chunks:
                stage(t - lag)
    for c in range(chunks):
        for copy in flight["blocks", c]:
            copy.wait_recv()
    for copy in started:
        copy.wait_send()


def fused(deltas, owners, master, momentum):
    blocks = owners.shape[1]
    slots, sub_rows, width = master.shape[2:]
    block_rows = deltas.shape[2] // blocks
    pod_count, rep_count = lax.axis_size("outer"), lax.axis_size("rep")
    owned_blocks, rank_own = ranks(owners, pod_count)
    mine = owned_blocks == lax.axis_index("outer")
    sel = (mine[:, None] & (rank_own[:, None] == jnp.arange(slots)[None, :])).astype(jnp.float32)
    clip_limit = 0.5 * math.sqrt(lax.axis_size("shard") * blocks * block_rows * width)
    copies = CHUNKS * (4 + 2 * (rep_count - 1) + 4 * (pod_count - 1) + 2 * (rep_count - 1) + 4)
    exchanged = lax.axis_size("shard") + rep_count + pod_count - 3
    copies += exchanged
    vmem = pl.BlockSpec(memory_space=pltpu.VMEM)
    bf16, f32 = jnp.bfloat16, jnp.float32
    out, new_momentum, new_master = pl.pallas_call(
        functools.partial(kernel, CHUNKS, rep_count, lax.axis_size("shard"), clip_limit),
        out_shape=(
            jax.ShapeDtypeStruct((SIDE, SIDE, block_rows, width), bf16),
            jax.ShapeDtypeStruct(master.shape[2:], f32),
            jax.ShapeDtypeStruct(master.shape[2:], f32),
        ),
        in_specs=[pl.BlockSpec(memory_space=pltpu.SMEM), vmem, vmem, vmem],
        out_specs=(vmem, vmem, vmem),
        scratch_shapes=[
            pltpu.VMEM((SIDE, block_rows, width), bf16),
            pltpu.VMEM((block_rows, width), f32),
            pltpu.VMEM((block_rows, width), bf16),
            pltpu.VMEM((block_rows, width), bf16),
            pltpu.VMEM((block_rows, width), bf16),
            pltpu.VMEM((rep_count - 1, sub_rows, width), bf16),
            pltpu.VMEM((blocks, sub_rows, width), bf16),
            pltpu.VMEM((blocks, sub_rows, width), bf16),
            pltpu.VMEM((pod_count - 1, sub_rows, width), bf16),
            pltpu.VMEM((4, 8, 128), f32),
            pltpu.VMEM((exchanged, 8, 128), f32),
            pltpu.SemaphoreType.DMA((copies,)),
            pltpu.SemaphoreType.DMA((copies,)),
        ],
        compiler_params=pltpu.CompilerParams(
            collective_id=0, has_side_effects=True, vmem_limit_bytes=60 * 1024 * 1024
        ),
    )(
        sel,
        deltas.reshape(SIDE, SIDE, block_rows, width),
        master.reshape(master.shape[2:]),
        momentum.reshape(momentum.shape[2:]),
    )
    return (
        out.reshape(blocks * block_rows, width),
        new_momentum.reshape(momentum.shape),
        new_master.reshape(master.shape),
    )


def local(deltas, owners, master, momentum):
    blocks_here = owners.shape[1]
    slot_count = master.shape[2]
    sub_rows = master.shape[3]
    row_width = deltas.shape[3]
    block_rows = deltas.shape[2] // blocks_here
    pod_count = lax.axis_size("outer")
    rep_count = lax.axis_size("rep")
    owned_blocks = owners[0, :, 0]
    pod_ids = jnp.arange(pod_count, dtype=jnp.int32)
    onehot = (owned_blocks[:, None] == pod_ids[None, :]).astype(jnp.int32)
    rank_all = jnp.cumsum(onehot, axis=0) - onehot
    rank_own = jnp.sum(rank_all * onehot, axis=1)
    slot_ids = jnp.arange(slot_count, dtype=jnp.int32)
    selector = (
        (owned_blocks[None, None, :] == pod_ids[:, None, None])
        & (rank_own[None, None, :] == slot_ids[None, :, None])
    ).astype(jnp.bfloat16)
    local_rows = deltas[0, 0].reshape(blocks_here, block_rows, row_width)
    block_sums = lax.psum_scatter(
        local_rows.astype(jnp.float32).astype(jnp.bfloat16), "rep", scatter_dimension=1, tiled=True
    ).astype(jnp.float32)
    block_sums = block_sums.astype(jnp.bfloat16)
    pod_part = jnp.einsum(
        "ojb,brw->ojrw", selector, block_sums, preferred_element_type=jnp.float32
    ).astype(jnp.bfloat16)
    arrived = lax.all_to_all(pod_part, "outer", split_axis=0, concat_axis=0, tiled=True)
    mean_share = jnp.sum(arrived.astype(jnp.float32), axis=0) / (pod_count * rep_count)
    local_sq = jnp.sum(mean_share * mean_share)
    total_sq = lax.psum(local_sq, ("outer", "rep", "shard"))
    total_entries = lax.axis_size("shard") * blocks_here * block_rows * row_width
    clip_limit = 0.5 * math.sqrt(total_entries)
    factor = jnp.minimum(1.0, clip_limit / jnp.sqrt(total_sq + 1e-06))
    step_part = factor * mean_share[None, None]
    new_momentum = 0.9 * momentum + step_part
    new_master = master - 0.7 * (step_part + 0.9 * new_momentum)
    params_here = new_master.astype(jnp.bfloat16)
    gathered = lax.all_gather(params_here, ("outer", "rep"), axis=0, tiled=True).reshape(
        pod_count, rep_count, slot_count, sub_rows, row_width
    )
    unpacked = jnp.einsum("ojb,oqjrw->bqrw", selector, gathered, preferred_element_type=jnp.float32)
    new_params = unpacked.astype(jnp.bfloat16).reshape(blocks_here * block_rows, row_width)
    return (new_params, new_momentum, new_master)


def solution(mesh):
    fits = mesh.shape["outer"] == SIDE * SIDE

    def body(deltas, owners, master, momentum):
        blocks = owners.shape[1]
        width, sub_rows = master.shape[4], master.shape[3]
        whole = width % (2 * CHUNKS * 128) == 0 and sub_rows % TILE == 0
        plan = fused if fits and whole and blocks == SIDE * SIDE else local
        return plan(deltas, owners, master, momentum)

    return jax.shard_map(
        body,
        mesh=mesh,
        in_specs=(
            P("outer", "rep", "shard", None),
            P("shard", None, None),
            P("outer", "shard", None, "rep", None),
            P("outer", "shard", None, "rep", None),
        ),
        out_specs=(
            P("shard", None),
            P("outer", "shard", None, "rep", None),
            P("outer", "shard", None, "rep", None),
        ),
        check_vma=False,
    )
```
